128 devices in a mesh: gz: 2 (over x_lo), gx: 2 (over core), gy: 32 (over z, y, x_hi).
Axes of the slice: x: 4 (x_hi: 2, x_lo: 2; x = x_hi * 2 + x_lo), y: 4, z: 4, core: 2. Of those that a mesh axis runs over, the one named last changes fastest.
Arguments:
- initial_field: float32 [128, 16, 4096], P('gz', 'gx', 'gy'), may hold values from -36 to 36
- plane_coupling: float32 [128, 16, 4096], P('gz', 'gx', 'gy'), may hold values from 0.06 to 0.24
- line_coupling: float32 [128, 16, 4096], P('gz', 'gx', 'gy'), may hold values from 1000 to 8000
- source: float32 [128, 16, 4096], P('gz', 'gx', 'gy'), may hold values from -4 to 4, as said below
- shift_table: float32 [8], replicated, may hold values from 0.5 to 1
- shift_index: int32 [4], replicated, may hold values from 0 to 7
Outputs:
- heated: float32 [128, 16, 4096], P('gz', 'gx', 'gy')
The draws below stay inside these ranges and needn't reach their ends.
Inputs may be any that keep to these rules, and one draw needn't show every extreme that they name: `shift_index`: one table row for each half-step. A heat source.
All inputs are finite; a program needn't handle non-finite values.
Results may differ from the reference program's by a relative error of at most 0.0003.
Values sent between devices are 32-bit elements; how exact they have to be, the bound alone decides.
No kernel may reach another device: no remote copies, remote signals or barrier semaphores. Data moves between devices by JAX's collectives and lax.ppermute only.
A program may use at most 64 MiB of HBM per device.

```python
import math
import jax
import jax.numpy as jnp
from jax import lax

SHIFTS = 8
HALF = 4
NX = 16
NY = 4096
NZ = 128


def draw_source(key, part):
    values = jnp.clip(jax.random.normal(key, (NZ, NX, NY), jnp.float32), -4.0, 4.0)
    return values


def place_ends(entries, rng, least, top_value):
    dims = entries.shape
    place = [jax.random.randint(jax.random.fold_in(rng, axis), (), 0, dims[axis]) for axis in range(len(dims))]
    entries = entries.at[tuple(place)].set(least)
    longest = dims.index(max(dims))
    place[longest] = (place[longest] + 1) % dims[longest]
    return entries.at[tuple(place)].set(top_value)


def block_scale(stream_key, dims, shards, low, top_value):
    level = 1.0
    for axis_at, blocks in shards:
        draws = jax.random.uniform(jax.random.fold_in(jax.random.fold_in(stream_key, 6), axis_at), (blocks,), jnp.float32, low / len(shards), top_value / len(shards))
        level = level * jnp.repeat(jnp.exp(draws), dims[axis_at] // blocks).reshape((-1,) + (1,) * (len(dims) - 1 - axis_at))
    return level


def centred(stream_key, dims, scale, most, shards=(), kind=jnp.bfloat16):
    loudness = block_scale(stream_key, dims, shards, -0.22, 0.18) if shards else 1.0
    array = jax.random.normal(stream_key, dims, jnp.float32) * scale * loudness
    return jnp.minimum(jnp.maximum(array, -most), most).astype(kind)


def setup_inputs(seed: int = 0) -> dict:
    seeds = jax.random.split(jax.random.key(seed), 7)
    initial_field = centred(seeds[0], (NZ, NX, NY), 6.0, 36.0, ((0, 2), (1, 2), (2, 32)), jnp.float32)
    plane_coupling = jnp.clip(jnp.exp(math.log(0.24) - 1.3862944 * jax.random.uniform(seeds[1], (NZ, NX, NY), jnp.float32) ** block_scale(seeds[1], (NZ, NX, NY), ((0, 2), (1, 2), (2, 32)), -0.2, 0.2)), 0.06, 0.24)
    line_coupling = jnp.clip(jnp.exp(math.log(8000.0) - 2.0794415 * jax.random.uniform(seeds[2], (NZ, NX, NY), jnp.float32) ** block_scale(seeds[2], (NZ, NX, NY), ((0, 2), (1, 2), (2, 32)), -0.2, 0.2)), 1000.0, 8000.0)
    source = draw_source(jax.random.fold_in(seeds[6], 71), 0)
    shift_table = jnp.clip(jax.random.uniform(seeds[4], (SHIFTS,), jnp.float32, 0.5, 1.0), 0.5, 1.0)
    shift_index = place_ends(jax.random.randint(seeds[5], (HALF,), 0, SHIFTS), jax.random.fold_in(seeds[5], 1), 0, SHIFTS - 1).astype(jnp.int32)
    return {"initial_field": initial_field, "plane_coupling": plane_coupling, "line_coupling": line_coupling, "source": source, "shift_table": shift_table, "shift_index": shift_index}


def lookup(shift_table, table_row):
    table_slots = jnp.arange(shift_table.shape[0], dtype=jnp.int32)
    return jnp.sum(jnp.where(table_slots == table_row, shift_table, jnp.zeros_like(shift_table)))


def plane_apply(current, coupling):
    padded = jnp.pad(current, ((0, 0), (1, 1), (1, 1)))
    beside_all = padded[:, 2:, 1:-1] + padded[:, :-2, 1:-1] + padded[:, 1:-1, 2:] + padded[:, 1:-1, :-2]
    return coupling * (beside_all - 4.0 * current)


def line_solve(explicit, line_coupling, shift_value):
    scaled = shift_value * line_coupling
    center = 1.0 + 2.0 * scaled

    def forward(previous, inputs):
        before_c, before_d = previous
        coupling, middle, right_side = inputs
        pivot_value = middle + coupling * before_c
        next_c = -coupling / pivot_value
        next_d = (right_side + coupling * before_d) / pivot_value
        return (next_c, next_d), (next_c, next_d)

    zero_plane = jnp.zeros_like(explicit[0])
    final_state, factors = lax.scan(forward, (zero_plane, zero_plane), (scaled, center, explicit))

    def backward(later_value, inputs):
        ratio, offset = inputs
        own_value = offset - ratio * later_value
        return own_value, own_value

    final_value, solved = lax.scan(backward, zero_plane, factors, reverse=True)
    return solved


def reference(initial_field, plane_coupling, line_coupling, source, shift_table, shift_index):
    current = initial_field
    for half_step in range(HALF):
        shift_value = lookup(shift_table, shift_index[half_step])
        explicit = current + shift_value * (plane_apply(current, plane_coupling) + source)
        current = line_solve(explicit, line_coupling, shift_value)
    return current
```

```python
import functools

import jax
import jax.numpy as jnp
from jax import lax
from jax.experimental import pallas as pl
from jax.experimental.pallas import tpu as pltpu
from jax.sharding import PartitionSpec as P


HALF = 4
L = 64
ROWS = 8
COLS = 128
SWAP = [(0, 1), (1, 0)]
F32 = jnp.float32


def lanes():
    return lax.broadcasted_iota(jnp.int32, (ROWS, COLS), 1)


def subs():
    return lax.broadcasted_iota(jnp.int32, (ROWS, COLS), 0)


def roll(x, by):
    by = by % COLS
    return x if by == 0 else pltpu.roll(x, by, 1)


def layer(m):
    return m + lax.axis_index("gz") * (L - 1 - 2 * m)


class Rows:
    def __init__(self):
        gx = lax.axis_index("gx")
        sub = subs()
        low = jnp.where(gx == 0, 1.0, 0.0).astype(F32)
        high = 1.0 - low
        self.top = sub == 0
        self.bottom = sub == ROWS - 1
        self.low = jnp.full((ROWS, COLS), low, F32)
        self.high = jnp.full((ROWS, COLS), high, F32)

    def around(self, own, oth):
        a, b = pltpu.roll(own, 1, 0), pltpu.roll(oth, 1, 0)
        c, d = pltpu.roll(own, ROWS - 1, 0), pltpu.roll(oth, ROWS - 1, 0)
        own_sum = jnp.where(self.top, self.high * b, a) + jnp.where(self.bottom, self.low * d, c)
        oth_sum = jnp.where(self.top, self.low * a, b) + jnp.where(self.bottom, self.high * c, d)
        return (
            own_sum + (roll(own, 1) + roll(own, -1)),
            oth_sum + (roll(oth, 1) + roll(oth, -1)),
        )


def factor(inverse, inverse_shift, rest):
    x = inverse * inverse_shift + rest
    g = 1.0 / (1.0 + x)
    return g, x * g


def meet(d, g, rest, far_d, far_rest):
    far_g = 1.0 - far_rest
    return (far_d + far_g * d) / (rest + far_rest - rest * far_rest)


def pack_edges_kernel(u, p, l, s, out):
    lane = lanes()
    for j in range(L // 2):
        acc = None
        for odd in range(2):
            k = layer(2 * j + odd)
            for a, ref in enumerate((u, p, l, s)):
                at = 64 * odd + 16 * a
                piece = roll(ref[k], 8 + at)
                acc = piece if acc is None else jnp.where(lane >= at, piece, acc)
        out[j] = acc


def pack_sides_kernel(u, p, l, s, z, out_b, out_c):
    lane = lanes()
    gz0 = lax.axis_index("gz") == 0
    for q in range(L // 4):
        left, right = None, None
        for half in range(2):
            for i in range(4):
                m = 4 * q + i
                for a, ref in enumerate((u, p, l, s)):
                    at = 64 * half + 16 * i + 4 * a
                    if half == 0:
                        base = 64 * (m % 2) + 16 * a
                        x = z[m // 2]
                        pl_, pr_ = roll(x, at - (base + 8)), roll(x, at - (base + 4))
                    else:
                        x = ref[layer(m)]
                        pl_, pr_ = roll(x, at), roll(x, at - 124)
                    left = pl_ if left is None else jnp.where(lane >= at, pl_, left)
                    right = pr_ if right is None else jnp.where(lane >= at, pr_, right)
        out_b[q] = jnp.where(gz0, left, right)
        out_c[q] = jnp.where(gz0, right, left)


def first_kernel(u, p, l, s, uo, po, lo, so, ish, g_out, c_out, d_out, pay):
    rows = Rows()
    shift = [ish[h] for h in range(HALF)]
    one = jnp.full((ROWS, COLS), 1.0, F32)
    zero = jnp.zeros((ROWS, COLS), F32)
    rest = [[one, one] for _ in range(HALF)]
    d = [zero, zero]
    for m in range(L):
        k = layer(m)
        fields = (u[k], uo[k])
        sums = rows.around(*fields)
        for x, (pr, lr, sr) in enumerate(((p, l, s), (po, lo, so))):
            inverse = 1.0 / lr[k]
            a1, a2 = inverse * pr[k], inverse * sr[k]
            c_out[0, x, m] = inverse
            c_out[1, x, m] = a1
            c_out[2, x, m] = a2
            f = fields[x] * (inverse * shift[0] - 4.0 * a1) + (a1 * sums[x] + a2)
            for h in range(HALF):
                g, rest[h][x] = factor(inverse, shift[h], rest[h][x])
                g_out[h, x, m] = g
                if h == 0:
                    d[x] = g * (d[x] + f)
                    d_out[x, m] = d[x]
    for x in range(2):
        pay[x] = d[x]
        for h in range(HALF):
            pay[2 + 2 * h + x] = rest[h][x]


def next_kernel(h, ish, g, c, d, rest, far_rest, far_d, d_out, pay, f_ref):
    rows = Rows()
    shift = ish[h]
    up = []
    for x in range(2):
        at = 2 + 2 * (h - 1) + x
        up.append(meet(d[x, L - 1], None, rest[at], far_d[x], far_rest[at]))
    for m in range(L - 1, -1, -1):
        up = [d[x, m] + g[h - 1, x, m] * up[x] for x in range(2)]
        sums = rows.around(*up)
        for x in range(2):
            inverse, a1, a2 = c[0, x, m], c[1, x, m], c[2, x, m]
            f_ref[x, m] = up[x] * (inverse * shift - 4.0 * a1) + (a1 * sums[x] + a2)
    now = [jnp.zeros((ROWS, COLS), F32)] * 2
    for m in range(L):
        for x in range(2):
            now[x] = g[h, x, m] * (now[x] + f_ref[x, m])
            d_out[x, m] = now[x]
    for x in range(2):
        pay[x] = now[x]


def last_kernel(g, d, rest, far_rest, far_d, edge, out):
    lane = lanes()
    side = (lane < 4) | (lane >= COLS - 4)
    at = 2 + 2 * (HALF - 1)
    up = meet(d[0, L - 1], None, rest[at], far_d[0], far_rest[at])
    for m in range(L - 1, -1, -1):
        up = d[0, m] + g[HALF - 1, 0, m] * up
        out[layer(m)] = jnp.where(side, edge[m], up)


def edge_kernel(u, p, l, s, uo, po, lo, so, z, zo, b, bo, cc, co, ish, out, g_ref, c_ref, d_ref, f_ref):
    rows = Rows()
    lane = lanes()
    within = lax.rem(lane, 64)
    gz0 = lax.axis_index("gz") == 0
    gy = lax.axis_index("gy")
    last = lax.axis_size("gy") - 1
    shift = [ish[h] for h in range(HALF)]
    in_right8 = within < 8
    in_right4 = (within >= 8) & (within < 12)
    in_left4 = (within >= 12) & (within < 16)
    in_left8 = (within >= 16) & (within < 24)
    far = lane >= 64
    keep = in_right8 | in_left8 | (in_right4 & (gy < last)) | (in_left4 & (gy > 0))
    one = jnp.full((ROWS, COLS), 1.0, F32)
    zero = jnp.zeros((ROWS, COLS), F32)
    rest = [[one, one] for _ in range(HALF)]
    d = [zero, zero]
    sources = ((u, p, l, s, z, b, cc), (uo, po, lo, so, zo, bo, co))
    for m in range(L):
        k = layer(m)
        got = []
        for x in range(2):
            refs = sources[x]
            zz = refs[4][m // 2]
            bb, cv = refs[5][m // 4], refs[6][m // 4]
            left, right = jnp.where(gz0, bb, cv), jnp.where(gz0, cv, bb)
            parts = []
            for a in range(4):
                raw = refs[a][k]
                base = 64 * (m % 2) + 16 * a
                slot = 16 * (m % 4) + 4 * a
                v8r = jnp.where(far, roll(zz, 64 - base), roll(raw, 8))
                v8l = jnp.where(far, roll(zz, 64 + 16 - (base + 8)), roll(raw, 16))
                v = jnp.where(in_left8, v8l, v8r)
                v = jnp.where(in_right4, roll(right, 8 - slot), v)
                v = jnp.where(in_left4, roll(left, 12 - slot), v)
                parts.append(jnp.where(keep, v, one if a == 2 else zero))
            got.append(parts)
        sums = rows.around(got[0][0], got[1][0])
        for x in range(2):
            uu, pp, ll, ss = got[x]
            inverse = 1.0 / ll
            a1, a2 = inverse * pp, inverse * ss
            c_ref[0, x, m] = inverse
            c_ref[1, x, m] = a1
            c_ref[2, x, m] = a2
            f = uu * (inverse * shift[0] - 4.0 * a1) + (a1 * sums[x] + a2)
            for h in range(HALF):
                g, rest[h][x] = factor(inverse, shift[h], rest[h][x])
                g_ref[h, x, m] = g
                if h == 0:
                    d[x] = g * (d[x] + f)
                    d_ref[x, m] = d[x]
    for h in range(HALF):
        up = [meet(d[x], None, rest[h][x], roll(d[x], 64), roll(rest[h][x], 64)) for x in range(2)]
        if h == HALF - 1:
            for m in range(L - 1, -1, -1):
                up[0] = d_ref[0, m] + g_ref[h, 0, m] * up[0]
                out[m] = jnp.where(lane < 64, roll(up[0], -16), roll(up[0], 120))
            break
        for m in range(L - 1, -1, -1):
            up = [d_ref[x, m] + g_ref[h, x, m] * up[x] for x in range(2)]
            sums = rows.around(*up)
            for x in range(2):
                inverse, a1, a2 = c_ref[0, x, m], c_ref[1, x, m], c_ref[2, x, m]
                f_ref[x, m] = up[x] * (inverse * shift[h + 1] - 4.0 * a1) + (a1 * sums[x] + a2)
        d = [zero, zero]
        for m in range(L):
            for x in range(2):
                d[x] = g_ref[h + 1, x, m] * (d[x] + f_ref[x, m])
                d_ref[x, m] = d[x]


def shape(*dims):
    return jax.ShapeDtypeStruct((*dims, ROWS, COLS), F32)


def call(body, outs, name, scratch=(), flops=1):
    vmem = pl.BlockSpec(memory_space=pltpu.VMEM)

    def run(*args):
        return pl.pallas_call(
            body,
            out_shape=outs,
            in_specs=[vmem] * len(args),
            out_specs=jax.tree.map(lambda _: vmem, outs),
            scratch_shapes=[pltpu.VMEM(s.shape, s.dtype) for s in scratch],
            compiler_params=pltpu.CompilerParams(vmem_limit_bytes=24 * 1024 * 1024),
            cost_estimate=pl.CostEstimate(flops=flops, bytes_accessed=0, transcendentals=0),
            name=name,
        )(*args)

    return run


def side_pairs(size, first, second):
    pairs = []
    for y in range(1, size):
        a, b = first * size + y - 1, second * size + y
        pairs += [(a, b), (b, a)]
    lone = (second * size, first * size + size - 1)
    return pairs + [(i, i) for i in lone]


def on_device(initial_field, plane_coupling, line_coupling, source, shift_table, shift_index):
    own = (initial_field, plane_coupling, line_coupling, source)
    slots = jnp.arange(shift_table.shape[0], dtype=jnp.int32)
    shifts = jnp.sum(
        jnp.where(slots[None] == shift_index[:, None], shift_table[None], 0.0), axis=1
    )
    ish = jnp.broadcast_to((1.0 / shifts)[:, None, None], (HALF, ROWS, COLS))
    oth = tuple(lax.ppermute(a, "gx", SWAP) for a in own)
    size = lax.axis_size("gy")
    zy = ("gz", "gy")

    z_out = call(pack_edges_kernel, shape(L // 2), "pack_edges")(*own)
    z_in = lax.ppermute(z_out, "gz", SWAP)
    g, c, d, pay = call(
        first_kernel, (shape(HALF, 2, L), shape(3, 2, L), shape(2, L), shape(10)), "first"
    )(*own, *oth, ish)
    rest = pay
    far = far_rest = lax.ppermute(pay, "gz", SWAP)

    out_b, out_c = call(pack_sides_kernel, (shape(L // 4), shape(L // 4)), "pack_sides")(*own, z_in)
    in_b = lax.ppermute(out_b, zy, side_pairs(size, 1, 0))
    in_c = lax.ppermute(out_c, zy, side_pairs(size, 0, 1))
    z_oth = lax.ppermute(z_in, "gx", SWAP)
    b_oth = lax.ppermute(in_b, "gx", SWAP)
    c_oth = lax.ppermute(in_c, "gx", SWAP)
    edge = call(
        edge_kernel,
        shape(L),
        "edge",
        (shape(HALF, 2, L), shape(3, 2, L), shape(2, L), shape(2, L)),
    )(*own, *oth, z_in, z_oth, in_b, b_oth, in_c, c_oth, ish)

    for h in range(1, HALF):
        d, pay = call(
            functools.partial(next_kernel, h),
            (shape(2, L), shape(2)),
            f"next_{h}",
            (shape(2, L),),
        )(ish, g, c, d, rest, far_rest, far)
        far = lax.ppermute(pay, "gz", SWAP)
    return call(last_kernel, shape(L), "last")(g, d, rest, far_rest, far, edge)


def solution(mesh):
    spec = P("gz", "gx", "gy")
    return jax.shard_map(
        on_device,
        mesh=mesh,
        in_specs=(spec,) * 4 + (P(), P()),
        out_specs=spec,
        check_vma=False,
    )
```

```python
import functools

import jax
import jax.numpy as jnp
from jax import lax
from jax.experimental import pallas as pl
from jax.experimental.pallas import tpu as pltpu
from jax.sharding import PartitionSpec as P


HALF = 4
L = 64
ROWS = 8
COLS = 128
SWAP = [(0, 1), (1, 0)]
F32 = jnp.float32


def lanes():
    return lax.broadcasted_iota(jnp.int32, (ROWS, COLS), 1)


def subs():
    return lax.broadcasted_iota(jnp.int32, (ROWS, COLS), 0)


def roll(x, by):
    if isinstance(by, int):
        by = by % COLS
        return x if by == 0 else pltpu.roll(x, by, 1)
    return pltpu.roll(x, lax.rem(by + 2 * COLS, COLS), 1)


def layer(m):
    return m + lax.axis_index("gz") * (L - 1 - 2 * m)


class Rows:
    def __init__(self):
        gx = lax.axis_index("gx")
        sub = subs()
        low = jnp.where(gx == 0, 1.0, 0.0).astype(F32)
        high = 1.0 - low
        self.top = sub == 0
        self.bottom = sub == ROWS - 1
        self.low = jnp.full((ROWS, COLS), low, F32)
        self.high = jnp.full((ROWS, COLS), high, F32)

    def around(self, own, oth):
        a, b = pltpu.roll(own, 1, 0), pltpu.roll(oth, 1, 0)
        c, d = pltpu.roll(own, ROWS - 1, 0), pltpu.roll(oth, ROWS - 1, 0)
        own_sum = jnp.where(self.top, self.high * b, a) + jnp.where(self.bottom, self.low * d, c)
        oth_sum = jnp.where(self.top, self.low * a, b) + jnp.where(self.bottom, self.high * c, d)
        return (
            own_sum + (roll(own, 1) + roll(own, -1)),
            oth_sum + (roll(oth, 1) + roll(oth, -1)),
        )


def factor(inverse, inverse_shift, rest):
    x = inverse * inverse_shift + rest
    g = 1.0 / (1.0 + x)
    return g, x * g


def meet(d, rest, far_d, far_rest):
    far_g = 1.0 - far_rest
    return (far_d + far_g * d) / (rest + far_rest - rest * far_rest)


def load_kernel(u_in, p_in, l_in, s_in, table_in, index_in, u, p, l, s, ish, out, table, index, sem):
    into = (u, p, l, s, table, index)
    copies = [
        pltpu.make_async_copy(src, dst, sem.at[i])
        for i, (src, dst) in enumerate(zip((u_in, p_in, l_in, s_in, table_in, index_in), into))
    ]
    for copy in copies:
        copy.start()
    lane = lanes()
    copies[5].wait()
    copies[4].wait()
    for h in range(HALF):
        ish[h] = 1.0 / jnp.full((ROWS, COLS), table[index[h]], F32)
    for copy in copies[:4]:
        copy.wait()
    gz = lax.axis_index("gz")
    for q in range(L // 4):
        acc = None
        for i in range(4):
            k = layer(4 * q + i)
            for a, ref in enumerate((u, p, l, s)):
                at = 32 * i + 8 * a
                piece = roll(ref[k], at + 8 * (1 - gz))
                acc = piece if acc is None else jnp.where(lane >= at, piece, acc)
        out[q] = acc


def pack_side_kernel(u, p, l, s, z, out):
    lane = lanes()
    gz = lax.axis_index("gz")
    for q in range(L // 4):
        acc = None
        for half in range(2):
            for i in range(4):
                for a, ref in enumerate((u, p, l, s)):
                    at = 64 * half + 16 * i + 4 * a
                    if half == 0:
                        piece = roll(z[q], at - (32 * i + 8 * a) - 4 * gz)
                    else:
                        piece = roll(ref[layer(4 * q + i)], at + 4 * gz)
                    acc = piece if acc is None else jnp.where(lane >= at, piece, acc)
        out[q] = acc


def first_kernel(u, p, l, s, uo, po, lo, so, ish, g_out, c_out, d_out, pay):
    rows = Rows()
    shift = [ish[h] for h in range(HALF)]
    one = jnp.full((ROWS, COLS), 1.0, F32)
    zero = jnp.zeros((ROWS, COLS), F32)
    rest = [[one, one] for _ in range(HALF)]
    d = [zero, zero]
    for m in range(L):
        k = layer(m)
        fields = (u[k], uo[k])
        sums = rows.around(*fields)
        for x, (pr, lr, sr) in enumerate(((p, l, s), (po, lo, so))):
            inverse = 1.0 / lr[k]
            a1, a2 = inverse * pr[k], inverse * sr[k]
            c_out[0, x, m] = inverse
            c_out[1, x, m] = a1
            c_out[2, x, m] = a2
            f = fields[x] * (inverse * shift[0] - 4.0 * a1) + (a1 * sums[x] + a2)
            for h in range(HALF):
                g, rest[h][x] = factor(inverse, shift[h], rest[h][x])
                g_out[h, x, m] = g
                if h == 0:
                    d[x] = g * (d[x] + f)
                    d_out[x, m] = d[x]
    for x in range(2):
        pay[x] = d[x]
        for h in range(HALF):
            pay[2 + 2 * h + x] = rest[h][x]


def next_kernel(h, ish, g, c, d, rest, far_rest, far_d, d_out, pay, f_ref):
    rows = Rows()
    shift = ish[h]
    up = []
    for x in range(2):
        at = 2 + 2 * (h - 1) + x
        up.append(meet(d[x, L - 1], rest[at], far_d[x], far_rest[at]))
    for m in range(L - 1, -1, -1):
        up = [d[x, m] + g[h - 1, x, m] * up[x] for x in range(2)]
        sums = rows.around(*up)
        for x in range(2):
            inverse, a1, a2 = c[0, x, m], c[1, x, m], c[2, x, m]
            f_ref[x, m] = up[x] * (inverse * shift - 4.0 * a1) + (a1 * sums[x] + a2)
    now = [jnp.zeros((ROWS, COLS), F32)] * 2
    for m in range(L):
        for x in range(2):
            now[x] = g[h, x, m] * (now[x] + f_ref[x, m])
            d_out[x, m] = now[x]
    for x in range(2):
        pay[x] = now[x]


def last_kernel(g, d, rest, far_rest, far, edge, out):
    lane = lanes()
    gz = lax.axis_index("gz")
    at = 2 + 2 * (HALF - 1)
    up = meet(d[0, L - 1], rest[at], far[0], far_rest[at])
    zone = jnp.where(gz == 0, 0, COLS - 4)
    here = (lane >= zone) & (lane < zone + 4)
    other = COLS - 4 - zone
    there = (lane >= other) & (lane < other + 4)
    for m in range(L - 1, -1, -1):
        up = d[0, m] + g[HALF - 1, 0, m] * up
        v = jnp.where(here, roll(edge[m], -4 + 120 * gz), up)
        got = roll(far[1 + m // 32], other - 4 * (m % 32))
        out[layer(m)] = jnp.where(there, got, v)


def edge_local_kernel(u, p, l, s, uo, po, lo, so, z, zo, out):
    gz = lax.axis_index("gz")
    far = lanes() >= 64
    for m in range(L):
        k = layer(m)
        for x, refs in enumerate(((u, p, l, s, z), (uo, po, lo, so, zo))):
            for a in range(4):
                near = roll(refs[a][k], 4 + 8 * gz)
                beyond = roll(refs[4][m // 4], 68 - 32 * (m % 4) - 8 * a)
                out[a, x, m] = jnp.where(far, beyond, near)


def edge_first_kernel(v_ref, b, bo, ish, g_ref, c_ref, d_ref, rest_ref, w_ref):
    rows = Rows()
    gz = lax.axis_index("gz")
    gy = lax.axis_index("gy")
    within = lax.rem(lanes(), 64)
    inner = (within >= 4) & (within < 12)
    zone = 12 * gz
    halo = (within >= zone) & (within < zone + 4)
    open_side = jnp.where(gz == 0, gy > 0, gy < lax.axis_size("gy") - 1)
    keep = inner | (halo & open_side)
    shift = [ish[h] for h in range(HALF)]
    one = jnp.full((ROWS, COLS), 1.0, F32)
    zero = jnp.zeros((ROWS, COLS), F32)
    for m in range(L):
        for x, ref in enumerate((b, bo)):
            for a in range(4):
                v = jnp.where(halo, roll(ref[m // 4], zone - 16 * (m % 4) - 4 * a), v_ref[a, x, m])
                w_ref[a, x, m] = jnp.where(keep, v, one if a == 2 else zero)
    rest = [[one, one] for _ in range(HALF)]
    d = [zero, zero]
    for m in range(L):
        fields = [w_ref[0, x, m] for x in range(2)]
        sums = rows.around(*fields)
        for x in range(2):
            inverse = 1.0 / w_ref[2, x, m]
            a1, a2 = inverse * w_ref[1, x, m], inverse * w_ref[3, x, m]
            c_ref[0, x, m] = inverse
            c_ref[1, x, m] = a1
            c_ref[2, x, m] = a2
            f = fields[x] * (inverse * shift[0] - 4.0 * a1) + (a1 * sums[x] + a2)
            for h in range(HALF):
                g, rest[h][x] = factor(inverse, shift[h], rest[h][x])
                g_ref[h, x, m] = g
                if h == 0:
                    d[x] = g * (d[x] + f)
                    d_ref[x, m] = d[x]
    for x in range(2):
        for h in range(HALF):
            rest_ref[2 * h + x] = rest[h][x]


def edge_rest_kernel(g_ref, c_ref, d_in, rest_ref, ish, out, back, d_ref, f_ref):
    rows = Rows()
    lane = lanes()
    gz = lax.axis_index("gz")
    zero = jnp.zeros((ROWS, COLS), F32)
    d = [d_in[x, L - 1] for x in range(2)]
    for h in range(HALF):
        source = d_in if h == 0 else d_ref
        rest = [rest_ref[2 * h + x] for x in range(2)]
        up = [meet(d[x], rest[x], roll(d[x], 64), roll(rest[x], 64)) for x in range(2)]
        if h == HALF - 1:
            acc = zero
            for m in range(L - 1, -1, -1):
                up[0] = source[0, m] + g_ref[h, 0, m] * up[0]
                out[m] = up[0]
                at = 4 * (m % 32)
                acc = jnp.where(lane < at + 4, roll(up[0], at - 68 - 4 * gz), acc)
                if m % 32 == 0:
                    back[m // 32] = acc
            break
        for m in range(L - 1, -1, -1):
            up = [source[x, m] + g_ref[h, x, m] * up[x] for x in range(2)]
            sums = rows.around(*up)
            for x in range(2):
                inverse, a1, a2 = c_ref[0, x, m], c_ref[1, x, m], c_ref[2, x, m]
                f_ref[x, m] = up[x] * (inverse * ish[h + 1] - 4.0 * a1) + (a1 * sums[x] + a2)
        d = [zero, zero]
        for m in range(L):
            for x in range(2):
                d[x] = g_ref[h + 1, x, m] * (d[x] + f_ref[x, m])
                d_ref[x, m] = d[x]


def shape(*dims):
    return jax.ShapeDtypeStruct((*dims, ROWS, COLS), F32)


VMEM = pl.BlockSpec(memory_space=pltpu.VMEM)
HBM = pl.BlockSpec(memory_space=pltpu.HBM)


def call(body, outs, scratch=(), flops=1, specs=VMEM, limit=16 * 1024):
    def run(*args):
        return pl.pallas_call(
            body,
            out_shape=outs,
            in_specs=[specs] * len(args),
            out_specs=jax.tree.map(lambda _: VMEM, outs),
            scratch_shapes=[
                pltpu.VMEM(s.shape, s.dtype) if isinstance(s, jax.ShapeDtypeStruct) else s
                for s in scratch
            ],
            compiler_params=pltpu.CompilerParams(vmem_limit_bytes=limit * 1024),
            cost_estimate=pl.CostEstimate(flops=flops, bytes_accessed=0, transcendentals=0),
        )(*args)

    return run


def side_pairs(size):
    pairs = []
    for y in range(1, size):
        pairs += [(size + y - 1, y), (y, size + y - 1)]
    return pairs + [(i, i) for i in (0, 2 * size - 1)]


def on_device(initial_field, plane_coupling, line_coupling, source, shift_table, shift_index):
    size = lax.axis_size("gy")
    whole = shape(L)
    *own, ish, z_out = call(
        load_kernel,
        tuple(pltpu.VMEM(w.shape, F32) for w in (whole,) * 4 + (shape(HALF), shape(L // 4))),
        (
            pltpu.SMEM(shift_table.shape, F32),
            pltpu.SMEM(shift_index.shape, jnp.int32),
            pltpu.SemaphoreType.DMA((6,)),
        ),
        specs=HBM,
    )(
        *(
            pltpu.with_memory_space_constraint(a, pltpu.HBM)
            for a in (
                initial_field, plane_coupling, line_coupling, source, shift_table, shift_index
            )
        )
    )
    z_in = lax.ppermute(z_out, "gz", SWAP)
    oth = [lax.ppermute(a, "gx", SWAP) for a in own]

    g, c, d, pay = call(
        first_kernel, (shape(HALF, 2, L), shape(3, 2, L), shape(2, L), shape(10))
    )(*own, *oth, ish)
    rest = pay
    far = far_rest = lax.ppermute(pay, "gz", SWAP)

    z_oth = lax.ppermute(z_in, "gx", SWAP)
    out_b = call(pack_side_kernel, shape(L // 4))(*own, z_in)
    in_b = lax.ppermute(out_b, ("gz", "gy"), side_pairs(size))
    b_oth = lax.ppermute(in_b, "gx", SWAP)

    def step(h, d, far):
        return call(
            functools.partial(next_kernel, h), (shape(2, L), shape(2)), (shape(2, L),)
        )(ish, g, c, d, rest, far_rest, far)

    d, pay = step(1, d, far)
    far = lax.ppermute(pay, "gz", SWAP)
    local = call(edge_local_kernel, shape(4, 2, L))(*own, *oth, z_in, z_oth)
    d, pay = step(2, d, far)
    far = lax.ppermute(pay, "gz", SWAP)
    eg, ec, ed, er = call(
        edge_first_kernel,
        (shape(HALF, 2, L), shape(3, 2, L), shape(2, L), shape(2 * HALF)),
        (shape(4, 2, L),),
    )(local, in_b, b_oth, ish)
    edge, back = call(
        edge_rest_kernel, (whole, shape(2)), (shape(2, L), shape(2, L))
    )(eg, ec, ed, er, ish)
    d, pay = step(3, d, far)
    far = lax.ppermute(jnp.concatenate([pay[:1], back]), "gz", SWAP)
    return call(last_kernel, whole)(g, d, rest, far_rest, far, edge)


def solution(mesh):
    spec = P("gz", "gx", "gy")

    return jax.shard_map(
        on_device, mesh=mesh, in_specs=(spec,) * 4 + (P(), P()), out_specs=spec, check_vma=False
    )
```

```python
import jax
import jax.numpy as jnp
from jax import lax
from jax.experimental import pallas as pl
from jax.experimental.pallas import tpu as pltpu
from jax.sharding import PartitionSpec as P


HALF = 4
CHUNK = 16
L = 64
ROWS = 8
COLS = 128
SWAP = [(0, 1), (1, 0)]
CROSS = [(i, 3 - i) for i in range(4)]
ZX = ("gz", "gx")
F32 = jnp.float32


def lanes():
    return lax.broadcasted_iota(jnp.int32, (ROWS, COLS), 1)


def subs():
    return lax.broadcasted_iota(jnp.int32, (ROWS, COLS), 0)


def roll(x, by):
    if isinstance(by, int):
        by = by % COLS
        return x if by == 0 else pltpu.roll(x, by, 1)
    return pltpu.roll(x, lax.rem(by + 2 * COLS, COLS), 1)


def layer(m):
    return m + lax.axis_index("gz") * (L - 1 - 2 * m)


def zone_side():
    return 1 - lax.axis_index("gz")


class Rows:
    def __init__(self):
        gx = lax.axis_index("gx")
        sub = subs()
        low = jnp.where(gx == 0, 1.0, 0.0).astype(F32)
        high = 1.0 - low
        self.top = sub == 0
        self.bottom = sub == ROWS - 1
        self.low = jnp.full((ROWS, COLS), low, F32)
        self.high = jnp.full((ROWS, COLS), high, F32)

    def beside(self, own, oth):
        a, b = pltpu.roll(own, 1, 0), pltpu.roll(oth, 1, 0)
        c, d = pltpu.roll(own, ROWS - 1, 0), pltpu.roll(oth, ROWS - 1, 0)
        return (
            (
                jnp.where(self.top, self.high * b, a),
                jnp.where(self.bottom, self.low * d, c),
                roll(own, 1),
                roll(own, -1),
            ),
            (
                jnp.where(self.top, self.low * a, b),
                jnp.where(self.bottom, self.high * c, d),
                roll(oth, 1),
                roll(oth, -1),
            ),
        )

    def around(self, own, oth):
        return tuple((n[0] + n[1]) + (n[2] + n[3]) for n in self.beside(own, oth))


def factor(inverse, inverse_shift, before):
    p, e = before
    e = e + (inverse * inverse_shift) * p
    after = p + e
    return p * (1.0 / after), (after, e)


def meet(d, rest, far_d, far_rest):
    far_g = 1.0 - far_rest
    return (far_d + far_g * d) / (rest + far_rest - rest * far_rest)


def forcing(own, around, inverse, a1, a2, shift):
    return own * (inverse * shift - 4.0 * a1) + (a1 * around + a2)


def explicit(rows, up, c, m, shift, f_ref, which=(0, 1)):
    sums = rows.around(*up)
    for x in which:
        f_ref[x, m] = forcing(up[x], sums[x], c[0, x, m], c[1, x, m], c[2, x, m], shift)


def reach(h, rows, shift, g, c, d, which):
    one = jnp.full((ROWS, COLS), 1.0, F32)
    zero = jnp.zeros((ROWS, COLS), F32)
    up, to, on = [zero] * 2, [one] * 2, [one] * 2
    total = [[zero] * 6 for _ in range(2)]
    for m in range(L - 1, -1, -1):
        for x in range(2):
            up[x] = d[x, m] + g[h, x, m] * up[x]
            to[x] = to[x] * g[h, x, m]
        around = rows.around(*up)
        beside = rows.beside(*to)
        for x in which:
            on[x] = on[x] * g[h + 1, x, m]
            inverse, a1, a2 = c[0, x, m], c[1, x, m], c[2, x, m]
            middle = inverse * shift - 4.0 * a1
            f = up[x] * middle + (a1 * around[x] + a2)
            weight = on[x] * a1
            add = [on[x] * f, on[x] * middle * to[x]] + [weight * n for n in beside[x]]
            total[x] = [t + v for t, v in zip(total[x], add)]
    return total


def reached(rows, total, last):
    beside = rows.beside(*last)
    found = []
    for x in range(2):
        t = total[x]
        value = None
        if t is not None:
            value = t(0) + t(1) * last[x]
            for i in range(4):
                value = value + t(2 + i) * beside[x][i]
        found.append(value)
    return found


def load_kernel(u_in, p_in, l_in, s_in, table_in, index_in, u, p, l, s, ish, out, table, index, sem):
    into = (u, p, l, s, table, index)
    copies = [
        pltpu.make_async_copy(src, dst, sem.at[i])
        for i, (src, dst) in enumerate(zip((u_in, p_in, l_in, s_in, table_in, index_in), into))
    ]
    for copy in copies:
        copy.start()
    lane = lanes()
    copies[5].wait()
    copies[4].wait()
    for h in range(HALF):
        ish[h] = 1.0 / jnp.full((ROWS, COLS), table[index[h]], F32)
    for copy in copies[:4]:
        copy.wait()
    side = zone_side()
    for q in range(L // 4):
        acc = None
        for i in range(4):
            k = layer(4 * q + i)
            for a, ref in enumerate((u, p, l, s)):
                at = 32 * i + 8 * a
                piece = roll(ref[k], at + 8 * (1 - side))
                acc = piece if acc is None else jnp.where(lane >= at, piece, acc)
        out[q] = acc


def pack_side_kernel(u, p, l, s, z, out):
    lane = lanes()
    side = zone_side()
    for q in range(L // 4):
        acc = None
        for half in range(2):
            for i in range(4):
                for a, ref in enumerate((u, p, l, s)):
                    at = 64 * half + 16 * i + 4 * a
                    if half == 0:
                        piece = roll(z[q], at - (32 * i + 8 * a) - 4 * side)
                    else:
                        piece = roll(ref[layer(4 * q + i)], at + 4 * side)
                    acc = piece if acc is None else jnp.where(lane >= at, piece, acc)
        out[q] = acc


def first_kernel(u, p, l, s, uo, po, lo, so, ish, g_out, c_out, d_out, rest_out, pay):
    rows = Rows()
    shift = [ish[h] for h in range(HALF)]
    one = jnp.full((ROWS, COLS), 1.0, F32)
    zero = jnp.zeros((ROWS, COLS), F32)
    rest = [[(one, one)] * 2 for _ in range(HALF)]
    d = [zero, zero]
    for m in range(L):
        k = layer(m)
        fields = (u[k], uo[k])
        sums = rows.around(*fields)
        for x, (pr, lr, sr) in enumerate(((p, l, s), (po, lo, so))):
            inverse = 1.0 / lr[k]
            a1, a2 = inverse * pr[k], inverse * sr[k]
            c_out[0, x, m] = inverse
            c_out[1, x, m] = a1
            c_out[2, x, m] = a2
            f = forcing(fields[x], sums[x], inverse, a1, a2, shift[0])
            for h in range(HALF):
                g, rest[h][x] = factor(inverse, shift[h], rest[h][x])
                g_out[h, x, m] = g
                if h == 0:
                    d[x] = g * (d[x] + f)
                    d_out[x, m] = d[x]
    total = reach(0, rows, shift[1], g_out, c_out, d_out, (0, 1))
    for x in range(2):
        pay[x] = d[x]
        for h in range(HALF):
            p, e = rest[h][x]
            rest_out[2 * h + x] = e / p
            pay[2 + 2 * h + x] = e / p
        for i in range(6):
            pay[10 + 6 * x + i] = total[x][i]


def middle_kernel(ish, g, c, d, rest, far, d_out, pay, f_ref, d_ref):
    rows = Rows()
    zero = jnp.zeros((ROWS, COLS), F32)

    def far_rest(h, x):
        return far[2 + 2 * h + 1 - x]

    up = [meet(d[x, L - 1], rest[x], far[1 - x], far_rest(0, x)) for x in range(2)]
    for m in range(L - 1, -1, -1):
        up = [d[x, m] + g[0, x, m] * up[x] for x in range(2)]
        if m == L - 1:
            last = up
        explicit(rows, up, c, m, ish[1], f_ref)
    now = [zero, zero]
    for m in range(L):
        for x in range(2):
            now[x] = g[1, x, m] * (now[x] + f_ref[x, m])
            d_ref[x, m] = now[x]
    far_d = reached(rows, [lambda i, x=x: far[10 + 6 * (1 - x) + i] for x in range(2)], last)
    up = [meet(now[x], rest[2 + x], far_d[x], far_rest(1, x)) for x in range(2)]
    for m in range(L - 1, -1, -1):
        up = [d_ref[x, m] + g[1, x, m] * up[x] for x in range(2)]
        explicit(rows, up, c, m, ish[2], f_ref)
    now = [zero, zero]
    for m in range(L):
        for x in range(2):
            now[x] = g[2, x, m] * (now[x] + f_ref[x, m])
            d_out[x, m] = now[x]
    total = reach(2, rows, ish[3], g, c, d_out, (1,))
    for x in range(2):
        pay[x] = now[x]
    for i in range(6):
        pay[2 + i] = total[1][i]


def last_kernel(ish, g, c, d, rest, far_rest, far, edge, out, field, f_ref, d_ref, sem):
    lane = lanes()
    rows = Rows()
    gz = lax.axis_index("gz")
    side = zone_side()
    up = [meet(d[x, L - 1], rest[4 + x], far[1 - x], far_rest[6 + 1 - x]) for x in range(2)]
    for m in range(L - 1, -1, -1):
        up = [d[x, m] + g[2, x, m] * up[x] for x in range(2)]
        if m == L - 1:
            last = up
        explicit(rows, up, c, m, ish[3], f_ref, (0,))
    now = jnp.zeros((ROWS, COLS), F32)
    for m in range(L):
        now = g[3, 0, m] * (now + f_ref[0, m])
        d_ref[m] = now
    far_d = reached(rows, [lambda i: far[2 + i], None], last)[0]
    up = meet(now, rest[6], far_d, far_rest[8 + 1])
    zone = jnp.where(side == 0, 0, COLS - 4)
    here = (lane >= zone) & (lane < zone + 4)
    other = COLS - 4 - zone
    there = (lane >= other) & (lane < other + 4)
    copies = []
    for m in range(L - 1, -1, -1):
        up = d_ref[m] + g[HALF - 1, 0, m] * up
        v = jnp.where(here, roll(edge[m], -4 + 120 * side), up)
        got = roll(far[8 + m // 32], other - 4 * (m % 32))
        field[layer(m)] = jnp.where(there, got, v)
        if m % CHUNK == 0:
            start = jnp.where(gz == 0, m, L - CHUNK - m)
            part = pl.ds(start, CHUNK)
            copies.append(pltpu.make_async_copy(field.at[part], out.at[part], sem.at[m // CHUNK]))
            copies[-1].start()
    for copy in copies:
        copy.wait()


def edge_local_kernel(u, p, l, s, uo, po, lo, so, z, zo, out):
    side = zone_side()
    far = lanes() >= 64
    for m in range(L):
        k = layer(m)
        for x, refs in enumerate(((u, p, l, s, z), (uo, po, lo, so, zo))):
            for a in range(4):
                near = roll(refs[a][k], 4 + 8 * side)
                beyond = roll(refs[4][m // 4], 68 - 32 * (m % 4) - 8 * a)
                out[a, x, m] = jnp.where(far, beyond, near)


def edge_first_kernel(v_ref, b, bo, ish, g_ref, c_ref, d_ref, rest_ref, w_ref):
    rows = Rows()
    side = zone_side()
    gy = lax.axis_index("gy")
    within = lax.rem(lanes(), 64)
    inner = (within >= 4) & (within < 12)
    zone = 12 * side
    halo = (within >= zone) & (within < zone + 4)
    open_side = jnp.where(side == 0, gy > 0, gy < lax.axis_size("gy") - 1)
    keep = inner | (halo & open_side)
    shift = [ish[h] for h in range(HALF)]
    one = jnp.full((ROWS, COLS), 1.0, F32)
    zero = jnp.zeros((ROWS, COLS), F32)
    for m in range(L):
        for x, ref in enumerate((b, bo)):
            for a in range(4):
                v = jnp.where(halo, roll(ref[m // 4], zone - 16 * (m % 4) - 4 * a), v_ref[a, x, m])
                w_ref[a, x, m] = jnp.where(keep, v, 1000.0 * one if a == 2 else zero)
    rest = [[(one, one)] * 2 for _ in range(HALF)]
    d = [zero, zero]
    for m in range(L):
        fields = [w_ref[0, x, m] for x in range(2)]
        sums = rows.around(*fields)
        for x in range(2):
            inverse = 1.0 / w_ref[2, x, m]
            a1, a2 = inverse * w_ref[1, x, m], inverse * w_ref[3, x, m]
            c_ref[0, x, m] = inverse
            c_ref[1, x, m] = a1
            c_ref[2, x, m] = a2
            f = forcing(fields[x], sums[x], inverse, a1, a2, shift[0])
            for h in range(HALF):
                g, rest[h][x] = factor(inverse, shift[h], rest[h][x])
                g_ref[h, x, m] = g
                if h == 0:
                    d[x] = g * (d[x] + f)
                    d_ref[x, m] = d[x]
    for x in range(2):
        for h in range(HALF):
            p, e = rest[h][x]
            rest_ref[2 * h + x] = e / p


def edge_rest_kernel(g_ref, c_ref, d_in, rest_ref, ish, pay, out, back, d_ref, f_ref):
    rows = Rows()
    lane = lanes()
    side = zone_side()
    zero = jnp.zeros((ROWS, COLS), F32)
    for i in range(8):
        back[i] = pay[i]
    d = [d_in[x, L - 1] for x in range(2)]
    for h in range(HALF):
        source = d_in if h == 0 else d_ref
        rest = [rest_ref[2 * h + x] for x in range(2)]
        up = [meet(d[x], rest[x], roll(d[x], 64), roll(rest[x], 64)) for x in range(2)]
        if h == HALF - 1:
            acc = zero
            for m in range(L - 1, -1, -1):
                up = [source[x, m] + g_ref[h, x, m] * up[x] for x in range(2)]
                out[m] = up[0]
                at = 4 * (m % 32)
                acc = jnp.where(lane < at + 4, roll(up[1], at - 68 - 4 * side), acc)
                if m % 32 == 0:
                    back[8 + m // 32] = acc
            break
        for m in range(L - 1, -1, -1):
            up = [source[x, m] + g_ref[h, x, m] * up[x] for x in range(2)]
            sums = rows.around(*up)
            for x in range(2):
                inverse, a1, a2 = c_ref[0, x, m], c_ref[1, x, m], c_ref[2, x, m]
                f_ref[x, m] = forcing(up[x], sums[x], inverse, a1, a2, ish[h + 1])
        d = [zero, zero]
        for m in range(L):
            for x in range(2):
                d[x] = g_ref[h + 1, x, m] * (d[x] + f_ref[x, m])
                d_ref[x, m] = d[x]


def shape(*dims):
    return jax.ShapeDtypeStruct((*dims, ROWS, COLS), F32)


VMEM = pl.BlockSpec(memory_space=pltpu.VMEM)
HBM = pl.BlockSpec(memory_space=pltpu.HBM)


def call(body, outs, scratch=(), flops=1, specs=VMEM, out_spec=VMEM):
    def run(*args):
        return pl.pallas_call(
            body,
            out_shape=outs,
            in_specs=[specs] * len(args),
            out_specs=jax.tree.map(lambda _: out_spec, outs),
            scratch_shapes=[
                pltpu.VMEM(s.shape, s.dtype) if isinstance(s, jax.ShapeDtypeStruct) else s
                for s in scratch
            ],
            compiler_params=pltpu.CompilerParams(vmem_limit_bytes=16 * 1024 * 1024),
            cost_estimate=pl.CostEstimate(flops=flops, bytes_accessed=0, transcendentals=0),
        )(*args)

    return run


def side_pairs(size):
    pairs = []
    for x in range(2):
        for y in range(1, size):
            a, b = x * size + y - 1, (3 - x) * size + y
            pairs += [(a, b), (b, a)]
        lone = (x * size + size - 1, (3 - x) * size)
        pairs += [(i, i) for i in lone]
    return pairs


def on_device(initial_field, plane_coupling, line_coupling, source, shift_table, shift_index):
    size = lax.axis_size("gy")
    whole = shape(L)
    *own, ish, z_out = call(
        load_kernel,
        tuple(pltpu.VMEM(w.shape, F32) for w in (whole,) * 4 + (shape(HALF), shape(L // 4))),
        (
            pltpu.SMEM(shift_table.shape, F32),
            pltpu.SMEM(shift_index.shape, jnp.int32),
            pltpu.SemaphoreType.DMA((6,)),
        ),
        specs=HBM,
    )(
        *(
            pltpu.with_memory_space_constraint(a, pltpu.HBM)
            for a in (
                initial_field, plane_coupling, line_coupling, source, shift_table, shift_index
            )
        )
    )
    z_oth = lax.ppermute(z_out, ZX, CROSS)
    oth = [lax.ppermute(a, "gx", SWAP) for a in own]

    steps = (shape(HALF, 2, L), shape(3, 2, L), shape(2, L))
    g, c, d, rest, pay = call(first_kernel, (*steps, shape(2 * HALF), shape(22)))(*own, *oth, ish)
    far_rest = lax.ppermute(pay, ZX, CROSS)

    z_in = lax.ppermute(z_oth, "gx", SWAP)
    out_b = call(pack_side_kernel, shape(L // 4))(*oth, z_oth)
    in_b = lax.ppermute(out_b, ("gz", "gx", "gy"), side_pairs(size))
    b_oth = lax.ppermute(in_b, "gx", SWAP)

    d, pay = call(
        middle_kernel, (shape(2, L), shape(8)), (shape(2, L), shape(2, L))
    )(ish, g, c, d, rest, far_rest)
    local = call(edge_local_kernel, shape(4, 2, L))(*own, *oth, z_in, z_oth)
    eg, ec, ed, er = call(
        edge_first_kernel, (*steps, shape(2 * HALF)), (shape(4, 2, L),)
    )(local, in_b, b_oth, ish)
    edge, pay = call(
        edge_rest_kernel, (whole, shape(10)), (shape(2, L), shape(2, L))
    )(eg, ec, ed, er, ish, pay)
    far = lax.ppermute(pay, ZX, CROSS)
    return call(
        last_kernel,
        whole,
        (whole, shape(2, L), whole, pltpu.SemaphoreType.DMA((L // CHUNK,))),
        out_spec=HBM,
    )(ish, g, c, d, rest, far_rest, far, edge)


def solution(mesh):
    spec = P("gz", "gx", "gy")

    return jax.shard_map(
        on_device, mesh=mesh, in_specs=(spec,) * 4 + (P(), P()), out_specs=spec, check_vma=False
    )
```

```python
import jax
import jax.numpy as jnp
from jax import lax
from jax.experimental import pallas as pl
from jax.experimental.pallas import tpu as pltpu
from jax.sharding import PartitionSpec as P


HALF = 4
CHUNK = 16
L = 64
ROWS = 8
COLS = 128
SWAP = [(0, 1), (1, 0)]
CROSS = [(i, 3 - i) for i in range(4)]
ZX = ("gz", "gx")
F32 = jnp.float32


def lanes():
    return lax.broadcasted_iota(jnp.int32, (ROWS, COLS), 1)


def subs():
    return lax.broadcasted_iota(jnp.int32, (ROWS, COLS), 0)


def roll(x, by):
    if isinstance(by, int):
        by = by % COLS
        return x if by == 0 else pltpu.roll(x, by, 1)
    return pltpu.roll(x, lax.rem(by + 2 * COLS, COLS), 1)


def layer(m):
    return m + lax.axis_index("gz") * (L - 1 - 2 * m)


def zone_side():
    return 1 - lax.axis_index("gz")


class Rows:
    def __init__(self):
        gx = lax.axis_index("gx")
        sub = subs()
        low = jnp.where(gx == 0, 1.0, 0.0).astype(F32)
        high = 1.0 - low
        self.top = sub == 0
        self.bottom = sub == ROWS - 1
        self.low = jnp.full((ROWS, COLS), low, F32)
        self.high = jnp.full((ROWS, COLS), high, F32)

    def beside(self, own, oth):
        a, b = pltpu.roll(own, 1, 0), pltpu.roll(oth, 1, 0)
        c, d = pltpu.roll(own, ROWS - 1, 0), pltpu.roll(oth, ROWS - 1, 0)
        return (
            (
                jnp.where(self.top, self.high * b, a),
                jnp.where(self.bottom, self.low * d, c),
                roll(own, 1),
                roll(own, -1),
            ),
            (
                jnp.where(self.top, self.low * a, b),
                jnp.where(self.bottom, self.high * c, d),
                roll(oth, 1),
                roll(oth, -1),
            ),
        )

    def around(self, own, oth):
        return tuple((n[0] + n[1]) + (n[2] + n[3]) for n in self.beside(own, oth))


def factor(inverse, inverse_shift, before):
    p, e = before
    e = e + (inverse * inverse_shift) * p
    after = p + e
    return p * (1.0 / after), (after, e)


def meet(d, rest, far_d, far_rest):
    far_g = 1.0 - far_rest
    return (far_d + far_g * d) / (rest + far_rest - rest * far_rest)


def forcing(own, around, inverse, a1, a2, shift):
    return own * (inverse * shift - 4.0 * a1) + (a1 * around + a2)


def explicit(rows, up, c, m, shift, f_ref, which=(0, 1)):
    sums = rows.around(*up)
    for x in which:
        f_ref[x, m] = forcing(up[x], sums[x], c[0, x, m], c[1, x, m], c[2, x, m], shift)


def reach(h, rows, shift, g, c, d, which):
    one = jnp.full((ROWS, COLS), 1.0, F32)
    zero = jnp.zeros((ROWS, COLS), F32)
    up, to, on = [zero] * 2, [one] * 2, [one] * 2
    total = [[zero] * 6 for _ in range(2)]
    for m in range(L - 1, -1, -1):
        for x in range(2):
            up[x] = d[x, m] + g[h, x, m] * up[x]
            to[x] = to[x] * g[h, x, m]
        around = rows.around(*up)
        beside = rows.beside(*to)
        for x in which:
            on[x] = on[x] * g[h + 1, x, m]
            inverse, a1, a2 = c[0, x, m], c[1, x, m], c[2, x, m]
            middle = inverse * shift - 4.0 * a1
            f = up[x] * middle + (a1 * around[x] + a2)
            weight = on[x] * a1
            add = [on[x] * f, on[x] * middle * to[x]] + [weight * n for n in beside[x]]
            total[x] = [t + v for t, v in zip(total[x], add)]
    return total


def reached(rows, total, last):
    beside = rows.beside(*last)
    found = []
    for x in range(2):
        t = total[x]
        value = None
        if t is not None:
            value = t(0) + t(1) * last[x]
            for i in range(4):
                value = value + t(2 + i) * beside[x][i]
        found.append(value)
    return found


def load_kernel(u_in, p_in, l_in, s_in, table_in, index_in, u, p, l, s, ish, out, table, index, sem):
    into = (u, p, l, s, table, index)
    copies = [
        pltpu.make_async_copy(src, dst, sem.at[i])
        for i, (src, dst) in enumerate(zip((u_in, p_in, l_in, s_in, table_in, index_in), into))
    ]
    for copy in copies:
        copy.start()
    lane = lanes()
    copies[5].wait()
    copies[4].wait()
    for h in range(HALF):
        ish[h] = 1.0 / jnp.full((ROWS, COLS), table[index[h]], F32)
    side = zone_side()
    for a, ref in enumerate((u, p, l, s)):
        copies[a].wait()
        mine = (lane // 8) % 4 == a
        for q in range(L // 4):
            acc = None
            for i in range(4):
                piece = roll(ref[layer(4 * q + i)], 32 * i + 8 * a + 8 * (1 - side))
                acc = piece if acc is None else jnp.where(lane >= 32 * i, piece, acc)
            out[q] = acc if a == 0 else jnp.where(mine, acc, out[q])


def pack_side_kernel(u, p, l, s, z, out):
    lane = lanes()
    side = zone_side()
    for q in range(L // 4):
        acc = None
        for pair in range(2):
            for half in range(2):
                for odd in range(2):
                    i = 2 * pair + odd
                    for a, ref in enumerate((u, p, l, s)):
                        at = 64 * pair + 32 * half + 16 * odd + 4 * a
                        if half == 0:
                            piece = roll(z[q], at - (32 * i + 8 * a) - 4 * side)
                        else:
                            piece = roll(ref[layer(4 * q + i)], at + 4 * side)
                        acc = piece if acc is None else jnp.where(lane >= at, piece, acc)
        out[q] = acc


def first_kernel(u, p, l, s, uo, po, lo, so, ish, g_out, c_out, d_out, rest_out, pay):
    rows = Rows()
    shift = [ish[h] for h in range(2)]
    one = jnp.full((ROWS, COLS), 1.0, F32)
    zero = jnp.zeros((ROWS, COLS), F32)
    rest = [[(one, one)] * 2 for _ in range(2)]
    d = [zero, zero]
    for m in range(L):
        k = layer(m)
        fields = (u[k], uo[k])
        sums = rows.around(*fields)
        for x, (pr, lr, sr) in enumerate(((p, l, s), (po, lo, so))):
            inverse = 1.0 / lr[k]
            a1, a2 = inverse * pr[k], inverse * sr[k]
            c_out[0, x, m] = inverse
            c_out[1, x, m] = a1
            c_out[2, x, m] = a2
            f = forcing(fields[x], sums[x], inverse, a1, a2, shift[0])
            for h in range(2):
                g, rest[h][x] = factor(inverse, shift[h], rest[h][x])
                g_out[h, x, m] = g
                if h == 0:
                    d[x] = g * (d[x] + f)
                    d_out[x, m] = d[x]
    total = reach(0, rows, shift[1], g_out, c_out, d_out, (0, 1))
    for x in range(2):
        pay[x] = d[x]
        for h in range(2):
            p, e = rest[h][x]
            rest_out[2 * h + x] = e / p
            pay[2 + 2 * h + x] = e / p
        for i in range(6):
            pay[6 + 6 * x + i] = total[x][i]


def middle_kernel(ish, g, c, d, rest, far, g_out, d_out, rest_out, pay, f_ref, d_ref):
    rows = Rows()
    zero = jnp.zeros((ROWS, COLS), F32)

    def far_rest(h, x):
        return far[2 + 2 * h + 1 - x]

    up = [meet(d[x, L - 1], rest[x], far[1 - x], far_rest(0, x)) for x in range(2)]
    for m in range(L - 1, -1, -1):
        up = [d[x, m] + g[0, x, m] * up[x] for x in range(2)]
        if m == L - 1:
            last = up
        explicit(rows, up, c, m, ish[1], f_ref)
    one = jnp.full((ROWS, COLS), 1.0, F32)
    after = [[(one, one)] * 2 for _ in range(2)]
    now = [zero, zero]
    for m in range(L):
        for x in range(2):
            for h in range(2):
                g_out[h, x, m], after[h][x] = factor(c[0, x, m], ish[2 + h], after[h][x])
            now[x] = g[1, x, m] * (now[x] + f_ref[x, m])
            d_ref[x, m] = now[x]
    far_d = reached(rows, [lambda i, x=x: far[6 + 6 * (1 - x) + i] for x in range(2)], last)
    up = [meet(now[x], rest[2 + x], far_d[x], far_rest(1, x)) for x in range(2)]
    for m in range(L - 1, -1, -1):
        up = [d_ref[x, m] + g[1, x, m] * up[x] for x in range(2)]
        explicit(rows, up, c, m, ish[2], f_ref)
    now = [zero, zero]
    for m in range(L):
        for x in range(2):
            now[x] = g_out[0, x, m] * (now[x] + f_ref[x, m])
            d_out[x, m] = now[x]
    total = reach(0, rows, ish[3], g_out, c, d_out, (1,))
    for x in range(2):
        pay[x] = now[x]
        for h in range(2):
            p, e = after[h][x]
            rest_out[2 * h + x] = e / p
            pay[8 + 2 * h + x] = e / p
    for i in range(6):
        pay[2 + i] = total[1][i]


def own_columns(side):
    lane = lanes()
    zone = (COLS - 4) * side
    return (lane >= zone) & (lane < zone + 4)


def finish_kernel(ish, g, c, d, rest, far, edge, out, f_ref, d_ref):
    rows = Rows()
    side = zone_side()
    here = own_columns(side)
    up = [meet(d[x, L - 1], rest[x], far[1 - x], far[8 + 1 - x]) for x in range(2)]
    for m in range(L - 1, -1, -1):
        up = [d[x, m] + g[0, x, m] * up[x] for x in range(2)]
        if m == L - 1:
            last = up
        explicit(rows, up, c, m, ish[3], f_ref, (0,))
    now = jnp.zeros((ROWS, COLS), F32)
    for m in range(L):
        now = g[1, 0, m] * (now + f_ref[0, m])
        d_ref[m] = now
    far_d = reached(rows, [lambda i: far[2 + i], None], last)[0]
    up = meet(now, rest[2], far_d, far[10 + 1])
    for m in range(L - 1, -1, -1):
        up = d_ref[m] + g[1, 0, m] * up
        out[layer(m)] = jnp.where(here, roll(edge[m], -4 + 120 * side), up)


def last_kernel(value, far, out, field, sem):
    gz = lax.axis_index("gz")
    other = 1 - zone_side()
    there = own_columns(other)
    copies = []
    for m in range(L - 1, -1, -1):
        got = roll(far[m // 32], (COLS - 4) * other - 4 * (m % 32))
        field[layer(m)] = jnp.where(there, got, value[layer(m)])
        if m % CHUNK == 0:
            start = jnp.where(gz == 0, m, L - CHUNK - m)
            part = pl.ds(start, CHUNK)
            copies.append(pltpu.make_async_copy(field.at[part], out.at[part], sem.at[m // CHUNK]))
            copies[-1].start()
    for copy in copies:
        copy.wait()


class Groups:
    def __init__(self):
        gx = lax.axis_index("gx")
        lane, sub = lanes(), subs()
        self.own = lane < 64
        self.near = lax.rem(lane, 64) < 32
        self.top = sub == 0
        self.bottom = sub == ROWS - 1
        low = jnp.where(gx == 0, 1.0, 0.0).astype(F32)
        self.before = jnp.where(self.own, 1.0 - low, low)
        self.after = jnp.where(self.own, low, 1.0 - low)

    def around(self, v):
        a, c = pltpu.roll(v, 1, 0), pltpu.roll(v, ROWS - 1, 0)
        across = roll(jnp.where(self.top, a, c), 64)
        before = jnp.where(self.top, self.before * across, a)
        after = jnp.where(self.bottom, self.after * across, c)
        return (before + after) + (roll(v, 1) + roll(v, -1))

    def far(self, v):
        return jnp.where(self.near, roll(v, -32), roll(v, 32))


def edge_local_kernel(u, p, l, s, uo, po, lo, so, z, zo, out, packed):
    side = zone_side()
    lane = lanes()
    near = lax.rem(lane, 64) < 32
    own = lane < 64
    for q in range(L // 4):
        across = roll(zo[q], 64)
        for i in range(4):
            packed[4 * q + i] = jnp.where(lane // 32 == i, z[q], across)
    for m in range(L):
        k = layer(m)
        for a, (ref, other) in enumerate(zip((u, p, l, s), (uo, po, lo, so))):
            here = jnp.where(own, roll(ref[k], 4 + 8 * side), roll(other[k], 68 + 8 * side))
            there = roll(packed[m], 36 - 32 * (m % 4) - 8 * a)
            out[a, m] = jnp.where(near, here, there)


def edge_first_kernel(v_ref, b, bo, ish, g_ref, c_ref, d_ref, rest_ref, w_ref, pairs, f_ref):
    groups = Groups()
    side = zone_side()
    gy = lax.axis_index("gy")
    within = lax.rem(lanes(), 32)
    inner = (within >= 4) & (within < 12)
    zone = 12 * side
    halo = (within >= zone) & (within < zone + 4)
    open_side = jnp.where(side == 0, gy > 0, gy < lax.axis_size("gy") - 1)
    keep = inner | (halo & open_side)
    shift = [ish[h] for h in range(HALF)]
    one = jnp.full((ROWS, COLS), 1.0, F32)
    zero = jnp.zeros((ROWS, COLS), F32)
    for q in range(L // 4):
        pairs[2 * q] = jnp.where(groups.own, b[q], roll(bo[q], 64))
        pairs[2 * q + 1] = jnp.where(groups.own, roll(b[q], 64), bo[q])
    for m in range(L):
        for a in range(4):
            side_columns = roll(pairs[m // 2], zone - 16 * (m % 2) - 4 * a)
            v = jnp.where(halo, side_columns, v_ref[a, m])
            w_ref[a, m] = jnp.where(keep, v, 1000.0 * one if a == 2 else zero)
    rest = [(one, one)] * HALF
    d = zero
    for m in range(L):
        field = w_ref[0, m]
        inverse = 1.0 / w_ref[2, m]
        a1, a2 = inverse * w_ref[1, m], inverse * w_ref[3, m]
        c_ref[0, m] = inverse
        c_ref[1, m] = a1
        c_ref[2, m] = a2
        f_ref[m] = forcing(field, groups.around(field), inverse, a1, a2, shift[0])
    for m in range(L):
        for h in range(HALF):
            g, rest[h] = factor(c_ref[0, m], shift[h], rest[h])
            g_ref[h, m] = g
            if h == 0:
                d = g * (d + f_ref[m])
                d_ref[m] = d
    for h in range(HALF):
        p, e = rest[h]
        rest_ref[h] = e / p


def edge_rest_kernel(g_ref, c_ref, d_in, rest_ref, ish, out, back, d_ref, f_ref):
    groups = Groups()
    lane = lanes()
    side = zone_side()
    zero = jnp.zeros((ROWS, COLS), F32)
    d = d_in[L - 1]
    for h in range(HALF):
        source = d_in if h == 0 else d_ref
        rest = rest_ref[h]
        up = meet(d, rest, groups.far(d), groups.far(rest))
        if h == HALF - 1:
            acc = zero
            for m in range(L - 1, -1, -1):
                up = source[m] + g_ref[h, m] * up
                out[m] = up
                at = 4 * (m % 32)
                acc = jnp.where(lane < at + 4, roll(up, at - 100 - 4 * side), acc)
                if m % 32 == 0:
                    back[m // 32] = acc
            break
        for m in range(L - 1, -1, -1):
            up = source[m] + g_ref[h, m] * up
            f_ref[m] = forcing(
                up, groups.around(up), c_ref[0, m], c_ref[1, m], c_ref[2, m], ish[h + 1]
            )
        d = zero
        for m in range(L):
            d = g_ref[h + 1, m] * (d + f_ref[m])
            d_ref[m] = d


def shape(*dims):
    return jax.ShapeDtypeStruct((*dims, ROWS, COLS), F32)


VMEM = pl.BlockSpec(memory_space=pltpu.VMEM)
HBM = pl.BlockSpec(memory_space=pltpu.HBM)


def call(body, outs, scratch=(), flops=1, specs=VMEM, out_spec=VMEM):
    def run(*args):
        return pl.pallas_call(
            body,
            out_shape=outs,
            in_specs=[specs] * len(args),
            out_specs=jax.tree.map(lambda _: out_spec, outs),
            scratch_shapes=[
                pltpu.VMEM(s.shape, s.dtype) if isinstance(s, jax.ShapeDtypeStruct) else s
                for s in scratch
            ],
            compiler_params=pltpu.CompilerParams(vmem_limit_bytes=16 * 1024 * 1024),
            cost_estimate=pl.CostEstimate(flops=flops, bytes_accessed=0, transcendentals=0),
        )(*args)

    return run


def side_pairs(size):
    pairs = []
    for x in range(2):
        for y in range(1, size):
            a, b = x * size + y - 1, (3 - x) * size + y
            pairs += [(a, b), (b, a)]
        lone = (x * size + size - 1, (3 - x) * size)
        pairs += [(i, i) for i in lone]
    return pairs


def on_device(initial_field, plane_coupling, line_coupling, source, shift_table, shift_index):
    size = lax.axis_size("gy")
    whole = shape(L)
    *own, ish, z_out = call(
        load_kernel,
        tuple(pltpu.VMEM(w.shape, F32) for w in (whole,) * 4 + (shape(HALF), shape(L // 4))),
        (
            pltpu.SMEM(shift_table.shape, F32),
            pltpu.SMEM(shift_index.shape, jnp.int32),
            pltpu.SemaphoreType.DMA((6,)),
        ),
        specs=HBM,
    )(
        *(
            pltpu.with_memory_space_constraint(a, pltpu.HBM)
            for a in (
                initial_field, plane_coupling, line_coupling, source, shift_table, shift_index
            )
        )
    )
    z_oth = lax.ppermute(z_out, ZX, CROSS)
    oth = [lax.ppermute(a, "gx", SWAP) for a in own]

    g, c, d, rest, pay = call(
        first_kernel, (shape(2, 2, L), shape(3, 2, L), shape(2, L), shape(4), shape(18))
    )(*own, *oth, ish)
    far = lax.ppermute(pay, ZX, CROSS)

    z_in = lax.ppermute(z_oth, "gx", SWAP)
    out_b = call(pack_side_kernel, shape(L // 4))(*oth, z_oth)
    in_b = lax.ppermute(out_b, ("gz", "gx", "gy"), side_pairs(size))
    b_oth = lax.ppermute(in_b, "gx", SWAP)

    g, d, rest, pay = call(
        middle_kernel,
        (shape(2, 2, L), shape(2, L), shape(4), shape(12)),
        (shape(2, L), shape(2, L)),
    )(ish, g, c, d, rest, far)
    far = lax.ppermute(pay, ZX, CROSS)
    local = call(edge_local_kernel, shape(4, L), (whole,))(*own, *oth, z_in, z_oth)
    eg, ec, ed, er = call(
        edge_first_kernel,
        (shape(HALF, L), shape(3, L), whole, shape(HALF)),
        (shape(4, L), shape(L // 2), whole),
    )(local, in_b, b_oth, ish)
    edge, back = call(edge_rest_kernel, (whole, shape(2)), (whole, whole))(eg, ec, ed, er, ish)
    back = lax.ppermute(back, ZX, CROSS)
    value = call(finish_kernel, whole, (shape(1, L), whole))(ish, g, c, d, rest, far, edge)
    return call(
        last_kernel, whole, (whole, pltpu.SemaphoreType.DMA((L // CHUNK,))), out_spec=HBM
    )(value, back)


def solution(mesh):
    spec = P("gz", "gx", "gy")

    return jax.shard_map(
        on_device, mesh=mesh, in_specs=(spec,) * 4 + (P(), P()), out_specs=spec, check_vma=False
    )
```

```python
import jax
import jax.numpy as jnp
from jax import lax
from jax.experimental import pallas as pl
from jax.experimental.pallas import tpu as pltpu
from jax.sharding import PartitionSpec as P


HALF = 4
CHUNK = 16
L = 64
ROWS = 8
COLS = 128
SWAP = [(0, 1), (1, 0)]
CROSS = [(i, 3 - i) for i in range(4)]
ZX = ("gz", "gx")
F32 = jnp.float32


def lanes():
    return lax.broadcasted_iota(jnp.int32, (ROWS, COLS), 1)


def subs():
    return lax.broadcasted_iota(jnp.int32, (ROWS, COLS), 0)


def roll(x, by):
    if isinstance(by, int):
        by = by % COLS
        return x if by == 0 else pltpu.roll(x, by, 1)
    return pltpu.roll(x, lax.rem(by + 2 * COLS, COLS), 1)


def layer(m):
    return m + lax.axis_index("gz") * (L - 1 - 2 * m)


def zone_side():
    return 1 - lax.axis_index("gz")


class Rows:
    def __init__(self):
        gx = lax.axis_index("gx")
        sub = subs()
        low = jnp.where(gx == 0, 1.0, 0.0).astype(F32)
        high = 1.0 - low
        self.top = sub == 0
        self.bottom = sub == ROWS - 1
        self.low = jnp.full((ROWS, COLS), low, F32)
        self.high = jnp.full((ROWS, COLS), high, F32)

    def beside(self, own, oth):
        a, b = pltpu.roll(own, 1, 0), pltpu.roll(oth, 1, 0)
        c, d = pltpu.roll(own, ROWS - 1, 0), pltpu.roll(oth, ROWS - 1, 0)
        return (
            (
                jnp.where(self.top, self.high * b, a),
                jnp.where(self.bottom, self.low * d, c),
                roll(own, 1),
                roll(own, -1),
            ),
            (
                jnp.where(self.top, self.low * a, b),
                jnp.where(self.bottom, self.high * c, d),
                roll(oth, 1),
                roll(oth, -1),
            ),
        )

    def around(self, own, oth):
        return tuple((n[0] + n[1]) + (n[2] + n[3]) for n in self.beside(own, oth))


def factor(inverse, inverse_shift, before):
    p, e = before
    e = e + (inverse * inverse_shift) * p
    after = p + e
    return p * (1.0 / after), (after, e)


def meet(d, rest, far_d, far_rest):
    far_g = 1.0 - far_rest
    return (far_d + far_g * d) / (rest + far_rest - rest * far_rest)


def forcing(own, around, inverse, a1, a2, shift):
    return own * (inverse * shift - 4.0 * a1) + (a1 * around + a2)


def explicit(rows, u_ref, c, shift, f_ref, which=(0, 1)):
    for m in range(L):
        up = [u_ref[x, m] for x in range(2)]
        sums = rows.around(*up)
        for x in which:
            f_ref[x, m] = forcing(up[x], sums[x], c[0, x, m], c[1, x, m], c[2, x, m], shift)


def reach(h, rows, shift, g, c, d, which, u_ref, t_ref):
    one = jnp.full((ROWS, COLS), 1.0, F32)
    zero = jnp.zeros((ROWS, COLS), F32)
    up, to, on = [zero] * 2, [one] * 2, [one] * 2
    total = [[zero] * 6 for _ in range(2)]
    for m in range(L - 1, -1, -1):
        for x in range(2):
            up[x] = d[x, m] + g[h, x, m] * up[x]
            to[x] = to[x] * g[h, x, m]
            u_ref[x, m] = up[x]
            t_ref[x, m] = to[x]
    for m in range(L - 1, -1, -1):
        up = [u_ref[x, m] for x in range(2)]
        to = [t_ref[x, m] for x in range(2)]
        around = rows.around(*up)
        beside = rows.beside(*to)
        for x in which:
            on[x] = on[x] * g[h + 1, x, m]
            inverse, a1, a2 = c[0, x, m], c[1, x, m], c[2, x, m]
            middle = inverse * shift - 4.0 * a1
            f = up[x] * middle + (a1 * around[x] + a2)
            weight = on[x] * a1
            add = [on[x] * f, on[x] * middle * to[x]] + [weight * n for n in beside[x]]
            total[x] = [t + v for t, v in zip(total[x], add)]
    return total


def reached(rows, total, last):
    beside = rows.beside(*last)
    found = []
    for x in range(2):
        t = total[x]
        value = None
        if t is not None:
            value = t(0) + t(1) * last[x]
            for i in range(4):
                value = value + t(2 + i) * beside[x][i]
        found.append(value)
    return found


def load_kernel(u_in, p_in, l_in, s_in, table_in, index_in, u, p, l, s, ish, out, table, index, sem):
    into = (u, p, l, s, table, index)
    copies = [
        pltpu.make_async_copy(src, dst, sem.at[i])
        for i, (src, dst) in enumerate(zip((u_in, p_in, l_in, s_in, table_in, index_in), into))
    ]
    for copy in copies:
        copy.start()
    lane = lanes()
    copies[5].wait()
    copies[4].wait()
    for h in range(HALF):
        ish[h] = 1.0 / jnp.full((ROWS, COLS), table[index[h]], F32)
    side = zone_side()
    for a, ref in enumerate((u, p, l, s)):
        copies[a].wait()
        mine = (lane // 8) % 4 == a
        for q in range(L // 4):
            acc = None
            for i in range(4):
                piece = roll(ref[layer(4 * q + i)], 32 * i + 8 * a + 8 * (1 - side))
                acc = piece if acc is None else jnp.where(lane >= 32 * i, piece, acc)
            out[q] = acc if a == 0 else jnp.where(mine, acc, out[q])


def pack_side_kernel(u, p, l, s, z, out):
    lane = lanes()
    side = zone_side()
    for q in range(L // 4):
        acc = None
        for pair in range(2):
            for half in range(2):
                for odd in range(2):
                    i = 2 * pair + odd
                    for a, ref in enumerate((u, p, l, s)):
                        at = 64 * pair + 32 * half + 16 * odd + 4 * a
                        if half == 0:
                            piece = roll(z[q], at - (32 * i + 8 * a) - 4 * side)
                        else:
                            piece = roll(ref[layer(4 * q + i)], at + 4 * side)
                        acc = piece if acc is None else jnp.where(lane >= at, piece, acc)
        out[q] = acc


def first_kernel(
    u, p, l, s, uo, po, lo, so, ish, g_out, c_out, d_out, rest_out, pay, f_ref, t_ref
):
    rows = Rows()
    shift = [ish[h] for h in range(2)]
    one = jnp.full((ROWS, COLS), 1.0, F32)
    zero = jnp.zeros((ROWS, COLS), F32)
    rest = [[(one, one)] * 2 for _ in range(2)]
    d = [zero, zero]
    for m in range(L):
        k = layer(m)
        fields = (u[k], uo[k])
        sums = rows.around(*fields)
        for x, (pr, lr, sr) in enumerate(((p, l, s), (po, lo, so))):
            inverse = 1.0 / lr[k]
            a1, a2 = inverse * pr[k], inverse * sr[k]
            c_out[0, x, m] = inverse
            c_out[1, x, m] = a1
            c_out[2, x, m] = a2
            f_ref[x, m] = forcing(fields[x], sums[x], inverse, a1, a2, shift[0])
    for m in range(L):
        for x in range(2):
            for h in range(2):
                g, rest[h][x] = factor(c_out[0, x, m], shift[h], rest[h][x])
                g_out[h, x, m] = g
                if h == 0:
                    d[x] = g * (d[x] + f_ref[x, m])
                    d_out[x, m] = d[x]
    total = reach(0, rows, shift[1], g_out, c_out, d_out, (0, 1), f_ref, t_ref)
    for x in range(2):
        pay[x] = d[x]
        for h in range(2):
            p, e = rest[h][x]
            rest_out[2 * h + x] = e / p
            pay[2 + 2 * h + x] = e / p
        for i in range(6):
            pay[6 + 6 * x + i] = total[x][i]


def middle_kernel(ish, g, c, d, rest, far, g_out, d_out, rest_out, pay, f_ref, d_ref, t_ref):
    rows = Rows()
    zero = jnp.zeros((ROWS, COLS), F32)

    def far_rest(h, x):
        return far[2 + 2 * h + 1 - x]

    up = [meet(d[x, L - 1], rest[x], far[1 - x], far_rest(0, x)) for x in range(2)]
    for m in range(L - 1, -1, -1):
        up = [d[x, m] + g[0, x, m] * up[x] for x in range(2)]
        for x in range(2):
            t_ref[x, m] = up[x]
        if m == L - 1:
            last = up
    explicit(rows, t_ref, c, ish[1], f_ref)
    one = jnp.full((ROWS, COLS), 1.0, F32)
    after = [[(one, one)] * 2 for _ in range(2)]
    now = [zero, zero]
    for m in range(L):
        for x in range(2):
            for h in range(2):
                g_out[h, x, m], after[h][x] = factor(c[0, x, m], ish[2 + h], after[h][x])
            now[x] = g[1, x, m] * (now[x] + f_ref[x, m])
            d_ref[x, m] = now[x]
    far_d = reached(rows, [lambda i, x=x: far[6 + 6 * (1 - x) + i] for x in range(2)], last)
    up = [meet(now[x], rest[2 + x], far_d[x], far_rest(1, x)) for x in range(2)]
    for m in range(L - 1, -1, -1):
        up = [d_ref[x, m] + g[1, x, m] * up[x] for x in range(2)]
        for x in range(2):
            t_ref[x, m] = up[x]
    explicit(rows, t_ref, c, ish[2], f_ref)
    now = [zero, zero]
    for m in range(L):
        for x in range(2):
            now[x] = g_out[0, x, m] * (now[x] + f_ref[x, m])
            d_out[x, m] = now[x]
    total = reach(0, rows, ish[3], g_out, c, d_out, (1,), f_ref, t_ref)
    for x in range(2):
        pay[x] = now[x]
        for h in range(2):
            p, e = after[h][x]
            rest_out[2 * h + x] = e / p
            pay[8 + 2 * h + x] = e / p
    for i in range(6):
        pay[2 + i] = total[1][i]


def own_columns(side):
    lane = lanes()
    zone = (COLS - 4) * side
    return (lane >= zone) & (lane < zone + 4)


def finish_kernel(ish, g, c, d, rest, far, edge, out, f_ref, d_ref, t_ref):
    rows = Rows()
    side = zone_side()
    here = own_columns(side)
    up = [meet(d[x, L - 1], rest[x], far[1 - x], far[8 + 1 - x]) for x in range(2)]
    for m in range(L - 1, -1, -1):
        up = [d[x, m] + g[0, x, m] * up[x] for x in range(2)]
        for x in range(2):
            t_ref[x, m] = up[x]
        if m == L - 1:
            last = up
    explicit(rows, t_ref, c, ish[3], f_ref, (0,))
    now = jnp.zeros((ROWS, COLS), F32)
    for m in range(L):
        now = g[1, 0, m] * (now + f_ref[0, m])
        d_ref[m] = now
    far_d = reached(rows, [lambda i: far[2 + i], None], last)[0]
    up = meet(now, rest[2], far_d, far[10 + 1])
    for m in range(L - 1, -1, -1):
        up = d_ref[m] + g[1, 0, m] * up
        out[layer(m)] = jnp.where(here, roll(edge[m], -4 + 120 * side), up)


def last_kernel(value, far, out, field, sem):
    gz = lax.axis_index("gz")
    other = 1 - zone_side()
    there = own_columns(other)
    copies = []
    for m in range(L - 1, -1, -1):
        got = roll(far[m // 32], (COLS - 4) * other - 4 * (m % 32))
        field[layer(m)] = jnp.where(there, got, value[layer(m)])
        if m % CHUNK == 0:
            start = jnp.where(gz == 0, m, L - CHUNK - m)
            part = pl.ds(start, CHUNK)
            copies.append(pltpu.make_async_copy(field.at[part], out.at[part], sem.at[m // CHUNK]))
            copies[-1].start()
    for copy in copies:
        copy.wait()


class Groups:
    def __init__(self):
        gx = lax.axis_index("gx")
        lane, sub = lanes(), subs()
        self.own = lane < 64
        self.near = lax.rem(lane, 64) < 32
        self.top = sub == 0
        self.bottom = sub == ROWS - 1
        low = jnp.where(gx == 0, 1.0, 0.0).astype(F32)
        self.before = jnp.where(self.own, 1.0 - low, low)
        self.after = jnp.where(self.own, low, 1.0 - low)

    def around(self, v):
        a, c = pltpu.roll(v, 1, 0), pltpu.roll(v, ROWS - 1, 0)
        across = roll(jnp.where(self.top, a, c), 64)
        before = jnp.where(self.top, self.before * across, a)
        after = jnp.where(self.bottom, self.after * across, c)
        return (before + after) + (roll(v, 1) + roll(v, -1))

    def far(self, v):
        return jnp.where(self.near, roll(v, -32), roll(v, 32))


def edge_local_kernel(u, p, l, s, uo, po, lo, so, z, zo, out, packed):
    side = zone_side()
    lane = lanes()
    near = lax.rem(lane, 64) < 32
    own = lane < 64
    for q in range(L // 4):
        across = roll(zo[q], 64)
        for i in range(4):
            packed[4 * q + i] = jnp.where(lane // 32 == i, z[q], across)
    for m in range(L):
        k = layer(m)
        for a, (ref, other) in enumerate(zip((u, p, l, s), (uo, po, lo, so))):
            here = jnp.where(own, roll(ref[k], 4 + 8 * side), roll(other[k], 68 + 8 * side))
            there = roll(packed[m], 36 - 32 * (m % 4) - 8 * a)
            out[a, m] = jnp.where(near, here, there)


def edge_first_kernel(v_ref, b, bo, ish, g_ref, c_ref, d_ref, rest_ref, w_ref, pairs, f_ref):
    groups = Groups()
    side = zone_side()
    gy = lax.axis_index("gy")
    within = lax.rem(lanes(), 32)
    inner = (within >= 4) & (within < 12)
    zone = 12 * side
    halo = (within >= zone) & (within < zone + 4)
    open_side = jnp.where(side == 0, gy > 0, gy < lax.axis_size("gy") - 1)
    keep = inner | (halo & open_side)
    shift = [ish[h] for h in range(HALF)]
    one = jnp.full((ROWS, COLS), 1.0, F32)
    zero = jnp.zeros((ROWS, COLS), F32)
    for q in range(L // 4):
        pairs[2 * q] = jnp.where(groups.own, b[q], roll(bo[q], 64))
        pairs[2 * q + 1] = jnp.where(groups.own, roll(b[q], 64), bo[q])
    for m in range(L):
        for a in range(4):
            side_columns = roll(pairs[m // 2], zone - 16 * (m % 2) - 4 * a)
            v = jnp.where(halo, side_columns, v_ref[a, m])
            w_ref[a, m] = jnp.where(keep, v, 1000.0 * one if a == 2 else zero)
    rest = [(one, one)] * HALF
    d = zero
    for m in range(L):
        field = w_ref[0, m]
        inverse = 1.0 / w_ref[2, m]
        a1, a2 = inverse * w_ref[1, m], inverse * w_ref[3, m]
        c_ref[0, m] = inverse
        c_ref[1, m] = a1
        c_ref[2, m] = a2
        f_ref[m] = forcing(field, groups.around(field), inverse, a1, a2, shift[0])
    for m in range(L):
        for h in range(HALF):
            g, rest[h] = factor(c_ref[0, m], shift[h], rest[h])
            g_ref[h, m] = g
            if h == 0:
                d = g * (d + f_ref[m])
                d_ref[m] = d
    for h in range(HALF):
        p, e = rest[h]
        rest_ref[h] = e / p


def edge_rest_kernel(g_ref, c_ref, d_in, rest_ref, ish, out, back, d_ref, f_ref):
    groups = Groups()
    lane = lanes()
    side = zone_side()
    zero = jnp.zeros((ROWS, COLS), F32)
    joints = []
    for h in range(HALF):
        rest, far_rest = rest_ref[h], groups.far(rest_ref[h])
        joints.append((1.0 - far_rest, 1.0 / (rest + far_rest - rest * far_rest)))
    d = d_in[L - 1]
    for h in range(HALF):
        source = d_in if h == 0 else d_ref
        far_g, inverse_joint = joints[h]
        up = (groups.far(d) + far_g * d) * inverse_joint
        if h == HALF - 1:
            acc = zero
            for m in range(L - 1, -1, -1):
                up = source[m] + g_ref[h, m] * up
                out[m] = up
                at = 4 * (m % 32)
                acc = jnp.where(lane < at + 4, roll(up, at - 100 - 4 * side), acc)
                if m % 32 == 0:
                    back[m // 32] = acc
            break
        for m in range(L - 1, -1, -1):
            up = source[m] + g_ref[h, m] * up
            f_ref[m] = forcing(
                up, groups.around(up), c_ref[0, m], c_ref[1, m], c_ref[2, m], ish[h + 1]
            )
        d = zero
        for m in range(L):
            d = g_ref[h + 1, m] * (d + f_ref[m])
            d_ref[m] = d


def shape(*dims):
    return jax.ShapeDtypeStruct((*dims, ROWS, COLS), F32)


VMEM = pl.BlockSpec(memory_space=pltpu.VMEM)
HBM = pl.BlockSpec(memory_space=pltpu.HBM)


def call(body, outs, scratch=(), flops=1, specs=VMEM, out_spec=VMEM):
    def run(*args):
        return pl.pallas_call(
            body,
            out_shape=outs,
            in_specs=[specs] * len(args),
            out_specs=jax.tree.map(lambda _: out_spec, outs),
            scratch_shapes=[
                pltpu.VMEM(s.shape, s.dtype) if isinstance(s, jax.ShapeDtypeStruct) else s
                for s in scratch
            ],
            compiler_params=pltpu.CompilerParams(vmem_limit_bytes=16 * 1024 * 1024),
            cost_estimate=pl.CostEstimate(flops=flops, bytes_accessed=0, transcendentals=0),
        )(*args)

    return run


def side_pairs(size):
    pairs = []
    for x in range(2):
        for y in range(1, size):
            a, b = x * size + y - 1, (3 - x) * size + y
            pairs += [(a, b), (b, a)]
        lone = (x * size + size - 1, (3 - x) * size)
        pairs += [(i, i) for i in lone]
    return pairs


def on_device(initial_field, plane_coupling, line_coupling, source, shift_table, shift_index):
    size = lax.axis_size("gy")
    whole = shape(L)
    *own, ish, z_out = call(
        load_kernel,
        tuple(pltpu.VMEM(w.shape, F32) for w in (whole,) * 4 + (shape(HALF), shape(L // 4))),
        (
            pltpu.SMEM(shift_table.shape, F32),
            pltpu.SMEM(shift_index.shape, jnp.int32),
            pltpu.SemaphoreType.DMA((6,)),
        ),
        specs=HBM,
    )(
        *(
            pltpu.with_memory_space_constraint(a, pltpu.HBM)
            for a in (
                initial_field, plane_coupling, line_coupling, source, shift_table, shift_index
            )
        )
    )
    z_oth = lax.ppermute(z_out, ZX, CROSS)
    oth = [lax.ppermute(a, "gx", SWAP) for a in own]

    g, c, d, rest, pay = call(
        first_kernel, (shape(2, 2, L), shape(3, 2, L), shape(2, L), shape(4), shape(18)),
        (shape(2, L), shape(2, L)),
    )(*own, *oth, ish)
    far = lax.ppermute(pay, ZX, CROSS)

    z_in = lax.ppermute(z_oth, "gx", SWAP)
    out_b = call(pack_side_kernel, shape(L // 4))(*oth, z_oth)
    in_b = lax.ppermute(out_b, ("gz", "gx", "gy"), side_pairs(size))
    b_oth = lax.ppermute(in_b, "gx", SWAP)

    g, d, rest, pay = call(
        middle_kernel,
        (shape(2, 2, L), shape(2, L), shape(4), shape(12)),
        (shape(2, L), shape(2, L), shape(2, L)),
    )(ish, g, c, d, rest, far)
    far = lax.ppermute(pay, ZX, CROSS)
    local = call(edge_local_kernel, shape(4, L), (whole,))(*own, *oth, z_in, z_oth)
    eg, ec, ed, er = call(
        edge_first_kernel,
        (shape(HALF, L), shape(3, L), whole, shape(HALF)),
        (shape(4, L), shape(L // 2), whole),
    )(local, in_b, b_oth, ish)
    edge, back = call(edge_rest_kernel, (whole, shape(2)), (whole, whole))(eg, ec, ed, er, ish)
    back = lax.ppermute(back, ZX, CROSS)
    value = call(finish_kernel, whole, (shape(1, L), whole, shape(2, L)))(
        ish, g, c, d, rest, far, edge
    )
    return call(
        last_kernel, whole, (whole, pltpu.SemaphoreType.DMA((L // CHUNK,))), out_spec=HBM
    )(value, back)


def solution(mesh):
    spec = P("gz", "gx", "gy")

    return jax.shard_map(
        on_device, mesh=mesh, in_specs=(spec,) * 4 + (P(), P()), out_specs=spec, check_vma=False
    )
```
